8 devices in a mesh: dp: 1 (over z), tp: 8 (over y, x, core).
Axes of the slice: x: 2, y: 2, z: 1, core: 2. Of those that a mesh axis runs over, the one named last changes fastest.
Arguments:
- hidden: bfloat16 [2, 4096, 4096], P('dp', 'tp')
- lengths: int32 [2], P('dp')
- ln_gain: float32 [2, 4096], replicated
- ln_bias: float32 [2, 4096], replicated
- w_query: bfloat16 [2, 4096, 16, 256], P(None, None, 'tp')
- w_key: bfloat16 [2, 4096, 16, 256], P(None, None, 'tp')
- w_value: bfloat16 [2, 4096, 16, 256], P(None, None, 'tp')
- w_attn_out: bfloat16 [2, 16, 256, 4096], P(None, 'tp')
- w_fc_in: bfloat16 [2, 4096, 16384], P(None, None, 'tp')
- b_fc_in: float32 [2, 16384], P(None, 'tp')
- w_fc_out: bfloat16 [2, 16384, 4096], P(None, 'tp')
- b_fc_out: float32 [2, 4096], replicated
Outputs:
- output 1: bfloat16 [2, 4096, 4096], P('dp', 'tp')
- output 2: bfloat16 [2, 2, 16, 4096, 256], P(None, 'dp', 'tp')
- output 3: bfloat16 [2, 2, 16, 4096, 256], P(None, 'dp', 'tp')
All inputs are finite; a program needn't handle non-finite values.
Results may differ from the reference program's by a relative error of at most 0.0136841.
Values are sent between devices in bfloat16 or wider.
A program may use at most 1 GiB of HBM per device.

```python
import jax
import jax.numpy as jnp
from jax import lax

D = 4096
HEADS = 16
HEAD = 256
FF = 16384
BATCH = 2
SEQ_LEN = 4096
LAYERS = 2
ROTARY_DIM = 64
LN_EPS = 1e-5


def setup_inputs(seed: int = 0, part: int = 0) -> dict:
    base_key = jax.random.key(seed)
    part_key = jax.random.fold_in(base_key, part)
    noise_key, drift_key, length_key = jax.random.split(part_key, 3)
    weight_keys = jax.random.split(base_key, 11)
    noise_part = jax.random.normal(noise_key, (BATCH, SEQ_LEN, D), jnp.float32)
    drift_part = jnp.cumsum(jax.random.normal(drift_key, (BATCH, SEQ_LEN, D), jnp.float32), axis=1) * SEQ_LEN ** -0.5
    hidden = (0.6 * noise_part + 0.8 * drift_part).astype(jnp.bfloat16)
    lengths = jax.random.randint(length_key, (BATCH,), 1, SEQ_LEN + 1, jnp.int32)
    attn_width = HEADS * HEAD

    def normal_weight(key_index, arr_shape, fan_in):
        return (jax.random.normal(weight_keys[key_index], arr_shape, jnp.float32) * fan_in ** -0.5).astype(jnp.bfloat16)

    return {
        "hidden": hidden,
        "lengths": lengths,
        "ln_gain": 1.0 + 0.3 * jax.random.normal(weight_keys[0], (LAYERS, D), jnp.float32),
        "ln_bias": 0.3 * jax.random.normal(weight_keys[1], (LAYERS, D), jnp.float32),
        "w_query": normal_weight(2, (LAYERS, D, HEADS, HEAD), D),
        "w_key": normal_weight(3, (LAYERS, D, HEADS, HEAD), D),
        "w_value": normal_weight(4, (LAYERS, D, HEADS, HEAD), D),
        "w_attn_out": normal_weight(5, (LAYERS, HEADS, HEAD, D), attn_width),
        "w_fc_in": normal_weight(6, (LAYERS, D, FF), D),
        "b_fc_in": jax.random.normal(weight_keys[7], (LAYERS, FF), jnp.float32),
        "w_fc_out": normal_weight(8, (LAYERS, FF, D), FF),
        "b_fc_out": 0.5 * jax.random.normal(weight_keys[9], (LAYERS, D), jnp.float32),
    }


def layer_norm(hidden_rows, gain_vec, bias_vec):
    rows_f32 = hidden_rows.astype(jnp.float32)
    row_mean = jnp.mean(rows_f32, axis=-1, keepdims=True)
    centered = rows_f32 - row_mean
    row_var = jnp.mean(centered * centered, axis=-1, keepdims=True)
    return (centered * lax.rsqrt(row_var + LN_EPS) * gain_vec + bias_vec).astype(jnp.bfloat16)


def rotary_tables(seq_full):
    positions = jnp.arange(seq_full).astype(jnp.float32)
    inv_freq = 10000.0 ** (-jnp.arange(0, ROTARY_DIM, 2).astype(jnp.float32) / ROTARY_DIM)
    angles = positions[:, None] * inv_freq[None, :]
    return jnp.cos(angles), jnp.sin(angles)


def apply_rotary(projected, cos_tab, sin_tab):
    lead_shape = projected.shape[:-1]
    pair_view = projected[..., :ROTARY_DIM].reshape(lead_shape + (ROTARY_DIM // 2, 2))
    even_part = pair_view[..., 0]
    odd_part = pair_view[..., 1]
    new_even = even_part * cos_tab - odd_part * sin_tab
    new_odd = odd_part * cos_tab + even_part * sin_tab
    rotated = jnp.stack([new_even, new_odd], axis=-1).reshape(lead_shape + (ROTARY_DIM,))
    return jnp.concatenate([rotated, projected[..., ROTARY_DIM:]], axis=-1)


def reference(hidden, lengths, ln_gain, ln_bias, w_query, w_key, w_value, w_attn_out, w_fc_in, b_fc_in, w_fc_out, b_fc_out):
    cos_tab, sin_tab = rotary_tables(SEQ_LEN)
    positions = jnp.arange(SEQ_LEN)
    allowed = (positions[None, :] <= positions[:, None])[None] & (positions[None, None, :] < lengths[:, None, None])
    score_scale = HEAD ** -0.5

    def one_layer(carry_hidden, layer_params):
        gain_vec, bias_vec, wq_l, wk_l, wv_l, wo_l, w_in_l, b_in_l, w_out_l, b_out_l = layer_params
        normed = layer_norm(carry_hidden, gain_vec, bias_vec)
        flat_rows = normed.reshape(BATCH * SEQ_LEN, D)

        def one_head(head_weights):
            wq_h, wk_h, wv_h = head_weights
            query_h = apply_rotary(jnp.dot(flat_rows, wq_h, preferred_element_type=jnp.float32).reshape(BATCH, SEQ_LEN, HEAD), cos_tab, sin_tab).astype(jnp.bfloat16)
            keys_h = apply_rotary(jnp.dot(flat_rows, wk_h, preferred_element_type=jnp.float32).reshape(BATCH, SEQ_LEN, HEAD), cos_tab, sin_tab).astype(jnp.bfloat16)
            values_h = jnp.dot(flat_rows, wv_h, preferred_element_type=jnp.float32).reshape(BATCH, SEQ_LEN, HEAD).astype(jnp.bfloat16)
            scores = jnp.einsum("bqe,bke->bqk", query_h.astype(jnp.float32), keys_h.astype(jnp.float32)) * score_scale
            scores = jnp.where(allowed, scores, -1e30)
            attn_probs = jax.nn.softmax(scores, axis=-1).astype(jnp.bfloat16)
            context = jnp.einsum("bqk,bke->bqe", attn_probs.astype(jnp.float32), values_h.astype(jnp.float32)).astype(jnp.bfloat16)
            return context, keys_h, values_h

        context, keys_h, values_h = lax.map(one_head, (jnp.transpose(wq_l, (1, 0, 2)), jnp.transpose(wk_l, (1, 0, 2)), jnp.transpose(wv_l, (1, 0, 2))))
        context_flat = jnp.transpose(context, (1, 2, 0, 3)).reshape(BATCH * SEQ_LEN, HEADS * HEAD)
        attn_out = jnp.dot(context_flat, wo_l.reshape(HEADS * HEAD, D), preferred_element_type=jnp.float32)
        fc_hidden = jax.nn.gelu(jnp.dot(flat_rows, w_in_l, preferred_element_type=jnp.float32) + b_in_l, approximate=True).astype(jnp.bfloat16)
        mlp_out = jnp.dot(fc_hidden, w_out_l, preferred_element_type=jnp.float32)
        new_rows = carry_hidden.reshape(BATCH * SEQ_LEN, D).astype(jnp.float32) + attn_out + mlp_out + b_out_l
        new_hidden = new_rows.astype(jnp.bfloat16).reshape(BATCH, SEQ_LEN, D)
        return new_hidden, (jnp.transpose(keys_h, (1, 0, 2, 3)), jnp.transpose(values_h, (1, 0, 2, 3)))

    final_hidden, caches = lax.scan(one_layer, hidden, (ln_gain, ln_bias, w_query, w_key, w_value, w_attn_out, w_fc_in, b_fc_in, w_fc_out, b_fc_out))
    return final_hidden, caches[0], caches[1]
```

```python
import functools

import jax
import jax.numpy as jnp
from jax import lax
from jax.experimental import pallas as pl
from jax.experimental.pallas import tpu as pltpu
from jax.sharding import Mesh, PartitionSpec as P


ROTARY_DIM = 64
LN_EPS = 1e-5
LANES = 128
PIECES = 2
LOG2E = 1.4426950408889634
MASKED = -1e30


def layer_norm(hidden_rows, gain_vec, bias_vec):
    rows_f32 = hidden_rows.astype(jnp.float32)
    row_mean = jnp.mean(rows_f32, axis=-1, keepdims=True)
    centered = rows_f32 - row_mean
    row_var = jnp.mean(centered * centered, axis=-1, keepdims=True)
    return (centered * lax.rsqrt(row_var + LN_EPS) * gain_vec + bias_vec).astype(jnp.bfloat16)


def norm_body(has_partial, waits, *refs):
    inputs = 5 if has_partial else 3
    refs = refs[:inputs] + refs[inputs + waits :]
    if has_partial:
        held_ref, part_ref, shift_ref, gain_ref, bias_ref, new_ref, normed_ref = refs
        rows = held_ref[...].astype(jnp.float32) + part_ref[...].astype(jnp.float32) + shift_ref[...]
        new_ref[...] = rows.astype(new_ref.dtype)
        rows = new_ref[...]
    else:
        held_ref, gain_ref, bias_ref, normed_ref = refs
        rows = held_ref[...]
    normed_ref[...] = layer_norm(rows, gain_ref[...], bias_ref[...])


def residual_norm(held, gain, bias, partial=None, shift=None, after=()):
    rows, d = held.shape
    block = min(rows, 128)
    row_spec = pl.BlockSpec((block, d), lambda i: (i, 0))
    vec_spec = pl.BlockSpec((1, d), lambda i: (0, 0))
    out = jax.ShapeDtypeStruct((rows, d), jnp.bfloat16)
    vec = lambda a: a.reshape(1, d)
    has_partial = partial is not None
    operands = [held] + ([partial, vec(shift)] if has_partial else []) + [vec(gain), vec(bias), *after]
    specs = [row_spec] + ([row_spec, vec_spec] if has_partial else []) + [vec_spec] * 2 + [pl.BlockSpec(memory_space=pl.ANY)] * len(after)
    return pl.pallas_call(
        functools.partial(norm_body, has_partial, len(after)),
        grid=(rows // block,),
        in_specs=specs,
        out_specs=[row_spec] * (1 + has_partial),
        out_shape=[out] * (1 + has_partial),
        name="residual_norm",
        cost_estimate=pl.CostEstimate(flops=12 * rows * d, bytes_accessed=8 * rows * d, transcendentals=0),
    )(*operands)


def rotary_lanes(seq_full):
    positions = jnp.arange(seq_full).astype(jnp.float32)
    inv_freq = 10000.0 ** (-jnp.arange(0, ROTARY_DIM, 2).astype(jnp.float32) / ROTARY_DIM)
    angles = positions[:, None] * jnp.repeat(inv_freq, 2)[None, :]
    rest = ((0, 0), (0, LANES - ROTARY_DIM))
    cos_tab = jnp.pad(jnp.cos(angles), rest, constant_values=1.0)
    sin_tab = jnp.pad(jnp.sin(angles), rest)
    even = (jnp.arange(LANES) % 2 == 0)[None, :]
    return cos_tab, jnp.where(even, -sin_tab, 0.0), jnp.where(even, 0.0, sin_tab)


def qkv_body(heads, head_dim, *refs):
    pieces = refs[:-9]
    wq_ref, wk_ref, wv_ref, cos_ref, up_ref, down_ref, q_ref, k_ref, v_ref = refs[-9:]
    rows = jnp.concatenate([piece[...] for piece in pieces], axis=0)
    for w_ref, o_ref, turned in ((wq_ref, q_ref, True), (wk_ref, k_ref, True), (wv_ref, v_ref, False)):
        projected = jnp.dot(rows, w_ref[...], preferred_element_type=jnp.float32)
        for head in range(heads):
            lo = head * head_dim
            if turned:
                first = projected[:, lo : lo + LANES]
                first = first * cos_ref[...] + pltpu.roll(first, LANES - 1, 1) * up_ref[...] + pltpu.roll(first, 1, 1) * down_ref[...]
                o_ref[head, :, :LANES] = first.astype(o_ref.dtype)
                o_ref[head, :, LANES:] = projected[:, lo + LANES : lo + head_dim].astype(o_ref.dtype)
            else:
                o_ref[head] = projected[:, lo : lo + head_dim].astype(o_ref.dtype)


def project_qkv(pieces, wq, wk, wv, tables, layer, heads, head_dim):
    devices, rows, d = pieces[0].shape
    block = rows * len(pieces)
    width = heads * head_dim
    weight_spec = pl.BlockSpec((None, d, width), lambda i: (layer, 0, 0), pipeline_mode=pl.Buffered(1))
    table_spec = pl.BlockSpec((block, LANES), lambda i: (i, 0))
    out_spec = pl.BlockSpec((heads, block, head_dim), lambda i: (0, i, 0))
    out = jax.ShapeDtypeStruct((heads, devices * block, head_dim), jnp.bfloat16)
    return pl.pallas_call(
        functools.partial(qkv_body, heads, head_dim),
        grid=(devices,),
        in_specs=[pl.BlockSpec((None, rows, d), lambda i: (i, 0, 0))] * len(pieces) + [weight_spec] * 3 + [table_spec] * 3,
        out_specs=[out_spec] * 3,
        out_shape=[out] * 3,
        name="project_qkv",
        cost_estimate=pl.CostEstimate(flops=6 * devices * block * d * width, bytes_accessed=2 * devices * block * d + 6 * d * width + 6 * devices * block * width, transcendentals=0),
        compiler_params=pltpu.CompilerParams(dimension_semantics=("arbitrary",), vmem_limit_bytes=60 * 1024 * 1024),
    )(*pieces, wq, wk, wv, *tables)


def attention_body(heads, head_dim, block, batch_idx, lengths_ref, q_ref, k_ref, v_ref, *rest):
    o_ref = rest[-1]
    length = lengths_ref[batch_idx]
    q_idx = pl.program_id(0)
    whole = jnp.minimum(q_idx, length // block)
    scale = LOG2E * head_dim**-0.5

    def scores_of(head, k_idx):
        keys = k_ref[head, pl.ds(pl.multiple_of(k_idx * block, block), block), :]
        return lax.dot_general(q_ref[head], keys, (((1,), (1,)), ((), ())), preferred_element_type=jnp.float32) * scale

    def values_of(head, k_idx):
        return v_ref[head, pl.ds(pl.multiple_of(k_idx * block, block), block), :]

    q_pos = q_idx * block + lax.broadcasted_iota(jnp.int32, (block, block), 0)
    k_pos = whole * block + lax.broadcasted_iota(jnp.int32, (block, block), 1)
    allowed = (k_pos <= q_pos) & (k_pos < length)
    state = []
    for head in range(heads):
        scores = jnp.where(allowed, scores_of(head, whole), MASKED)
        top = jnp.max(scores, axis=1, keepdims=True)
        probs = jnp.exp2(scores - top)
        total = jnp.sum(probs, axis=1, keepdims=True)
        acc = jnp.dot(probs.astype(jnp.bfloat16), values_of(head, whole), preferred_element_type=jnp.float32)
        state.append((top, total, acc))

    def step(k_idx, state):
        out = []
        for head, (top, total, acc) in enumerate(state):
            scores = scores_of(head, k_idx)
            new_top = jnp.maximum(top, jnp.max(scores, axis=1, keepdims=True))
            probs = jnp.exp2(scores - new_top)
            shrink = jnp.exp2(top - new_top)
            total = total * shrink + jnp.sum(probs, axis=1, keepdims=True)
            acc = acc * shrink + jnp.dot(probs.astype(jnp.bfloat16), values_of(head, k_idx), preferred_element_type=jnp.float32)
            out.append((new_top, total, acc))
        return tuple(out)

    state = lax.fori_loop(0, whole, step, tuple(state))
    for head, (_, total, acc) in enumerate(state):
        o_ref[:, head * head_dim : (head + 1) * head_dim] = (acc / total).astype(o_ref.dtype)


def causal_attention(lengths, query_all, keys_all, values_all, batch_idx, block, after=()):
    heads, seq, head_dim = query_all.shape
    whole_spec = pl.BlockSpec((heads, seq, head_dim), lambda i, *_: (0, 0, 0))
    return pl.pallas_call(
        functools.partial(attention_body, heads, head_dim, block, batch_idx),
        grid_spec=pltpu.PrefetchScalarGridSpec(
            num_scalar_prefetch=1,
            grid=(seq // block,),
            in_specs=[pl.BlockSpec((heads, block, head_dim), lambda i, *_: (0, i, 0)), whole_spec, whole_spec] + [pl.BlockSpec(memory_space=pl.ANY)] * len(after),
            out_specs=pl.BlockSpec((block, heads * head_dim), lambda i, *_: (i, 0)),
        ),
        out_shape=jax.ShapeDtypeStruct((seq, heads * head_dim), jnp.bfloat16),
        name="causal_attention",
        cost_estimate=pl.CostEstimate(flops=4 * heads * seq * seq * head_dim, bytes_accessed=8 * heads * seq * head_dim, transcendentals=heads * seq * seq // 2),
        compiler_params=pltpu.CompilerParams(dimension_semantics=("arbitrary",), vmem_limit_bytes=60 * 1024 * 1024),
    )(lengths, query_all, keys_all, values_all, *after)


def out_body(ctx_ref, fc_ref, wo_ref, w_ref, o_ref, send_ref, recv_ref, send_sem, recv_sem):
    n, h, side = (pl.program_id(i) for i in range(3))
    halves = pl.num_programs(1)
    sibling = 1 - lax.axis_index("core")
    slot = n * halves + h

    def exchange():
        return pltpu.make_async_remote_copy(
            src_ref=send_ref, dst_ref=recv_ref.at[slot], send_sem=send_sem, recv_sem=recv_sem.at[slot], device_id={"core": sibling}, device_id_type=pl.DeviceIdType.MESH
        )

    @pl.when((n == 0) & (h == 0) & (side == 0))
    def _():
        barrier = pltpu.get_barrier_semaphore()
        pl.semaphore_signal(barrier, inc=1, device_id={"core": sibling}, device_id_type=pl.DeviceIdType.MESH)
        pl.semaphore_wait(barrier, 1)

    @pl.when(side == 1)
    def _():
        exchange().start()

    groups, rows, width = ctx_ref.shape
    total = jnp.dot(fc_ref[...].reshape(groups * rows, fc_ref.shape[-1]), w_ref[...], preferred_element_type=jnp.float32)
    total += jnp.dot(ctx_ref[...].reshape(groups * rows, width), wo_ref[...], preferred_element_type=jnp.float32)

    @pl.when(side == 0)
    def _():
        send_ref[...] = total.astype(send_ref.dtype)

    @pl.when(side == 1)
    def _():
        exchange().wait()
        o_ref[...] = (total + recv_ref[slot].astype(jnp.float32)).astype(o_ref.dtype).reshape(o_ref.shape)


def project_out(context, fc_hidden, wo, w_out, layer, piece, collective_id):
    chips, cores, _, rows, width = context.shape
    ff = fc_hidden.shape[-1]
    d = wo.shape[-1]
    group = min(chips, max(1, 1024 // rows))
    cols = 1024
    halves = chips // group
    block = group * rows

    def core_of(side):
        return lax.rem(lax.axis_index("core") + 1 + side, 2)

    work = chips * cores * rows
    return pl.pallas_call(
        out_body,
        grid=(d // cols, halves, cores),
        in_specs=[
            pl.BlockSpec((group, None, None, rows, width), lambda n, h, s: (h, core_of(s), piece, 0, 0)),
            pl.BlockSpec((group, None, None, rows, ff), lambda n, h, s: (h, core_of(s), 0, 0, 0)),
            pl.BlockSpec((None, width, cols), lambda n, h, s: (layer, 0, n)),
            pl.BlockSpec((None, ff, cols), lambda n, h, s: (layer, 0, n)),
        ],
        out_specs=pl.BlockSpec((group, rows, cols), lambda n, h, s: (h, 0, n)),
        out_shape=jax.ShapeDtypeStruct((chips, rows, d), jnp.bfloat16),
        scratch_shapes=[
            pltpu.VMEM((block, cols), jnp.bfloat16),
            pltpu.VMEM((d // cols * halves, block, cols), jnp.bfloat16),
            pltpu.SemaphoreType.DMA,
            pltpu.SemaphoreType.DMA((d // cols * halves,)),
        ],
        name="project_out",
        cost_estimate=pl.CostEstimate(flops=2 * work * (ff + width) * d, bytes_accessed=2 * (work * (ff + width + d) + (ff + width) * d), transcendentals=0),
        compiler_params=pltpu.CompilerParams(dimension_semantics=("arbitrary",) * 3, vmem_limit_bytes=63 * 1024 * 1024, collective_id=collective_id, has_side_effects=True),
    )(context, fc_hidden, wo, w_out)


def solution(mesh):
    tp_size = mesh.shape["tp"]
    mesh = Mesh(mesh.devices.reshape(mesh.shape["dp"], tp_size // 2, 2), ("dp", "chip", "core"))
    tp = ("chip", "core")

    def device_step(hidden, lengths, ln_gain, ln_bias, w_query, w_key, w_value, w_attn_out, w_fc_in, b_fc_in, w_fc_out, b_fc_out):
        batch, rows_own, d = hidden.shape
        layers, _, heads, head_dim = w_query.shape
        seq_full = rows_own * tp_size
        tables = rotary_lanes(seq_full)
        wq, wk, wv = (w.reshape(layers, d, heads * head_dim) for w in (w_query, w_key, w_value))
        wo = w_attn_out.reshape(layers, heads * head_dim, d)
        chips = tp_size // 2

        def pieces_of(layer, b):
            return PIECES if (layer, b) in ((0, 0), (layers - 1, batch - 1)) else 1

        def gather(normed, layer, b):
            count = pieces_of(layer, b)
            rows = rows_own // count
            gathered = []
            for piece in range(count):
                gathered.append(lax.all_gather(normed[piece * rows : (piece + 1) * rows], tp, axis=0))
            return gathered

        def fc_in(rows, layer):
            return jax.nn.gelu(jnp.einsum("ntd,df->ntf", rows, w_fc_in[layer], preferred_element_type=jnp.float32) + b_fc_in[layer], approximate=True).astype(jnp.bfloat16)

        held = [hidden[b] for b in range(batch)]
        normed = [residual_norm(held[b], ln_gain[0], ln_bias[0])[0] for b in range(batch)]
        gathered = [gather(normed[b], 0, b) for b in range(batch)]
        cache_k = []
        cache_v = []
        waiting = None
        for layer, b in [(layer, b) for layer in range(layers) for b in range(batch)]:
            pieces = pieces_of(layer, b)
            rows = rows_own // pieces
            first_fc = fc_in(gathered[b][0], layer)
            query_all, keys_all, values_all = project_qkv(gathered[b], wq, wk, wv, tables, layer, heads, head_dim)
            cache_k.append(keys_all)
            cache_v.append(values_all)
            after = [first_fc]
            if waiting is not None and waiting[0] < layers - 1:
                up, prompt, sums = waiting
                held[prompt], normed[prompt] = residual_norm(held[prompt], ln_gain[up + 1], ln_bias[up + 1], sums, b_fc_out[up], [first_fc, query_all])
                gathered[prompt] = gather(normed[prompt], up + 1, prompt)
                after.append(normed[prompt])
            elif waiting is not None:
                held[waiting[1]] = (held[waiting[1]].astype(jnp.float32) + waiting[2].astype(jnp.float32) + b_fc_out[layer]).astype(jnp.bfloat16)
            context = causal_attention(lengths, query_all, keys_all, values_all, b, rows_own, after)
            context = context.reshape(chips, 2, pieces, rows, heads * head_dim)
            reduced = []
            part = None
            for piece in range(pieces):
                if piece == 0:
                    fc = first_fc
                else:
                    source, _ = lax.optimization_barrier((gathered[b][piece], part))
                    fc = fc_in(source, layer)
                fc = fc.reshape(chips, 2, 1, rows, -1)
                part = project_out(context, fc, wo, w_fc_out, layer, piece, (layer * batch + b) * PIECES + piece)
                reduced.append(lax.psum_scatter(part, "chip", scatter_dimension=0))
            waiting = (layer, b, jnp.concatenate(reduced, axis=0))
        layer, b, sums = waiting
        held[b] = (held[b].astype(jnp.float32) + sums.astype(jnp.float32) + b_fc_out[layer]).astype(jnp.bfloat16)
        cache_shape = (layers, batch, heads, seq_full, head_dim)
        return jnp.stack(held), jnp.stack(cache_k).reshape(cache_shape), jnp.stack(cache_v).reshape(cache_shape)

    head_cols = P(None, None, tp, None)
    cache_spec = P(None, "dp", tp, None, None)
    hidden_spec = P("dp", tp, None)
    return jax.shard_map(device_step, mesh=mesh, in_specs=(hidden_spec, P("dp"), P(), P(), head_cols, head_cols, head_cols, P(None, tp, None, None), P(None, None, tp), P(None, tp), P(None, tp, None), P()), out_specs=(hidden_spec, cache_spec, cache_spec), check_vma=False)
```

```python
import functools
import math

import jax
import jax.numpy as jnp
from jax import lax
from jax.experimental import pallas as pl
from jax.experimental.pallas import tpu as pltpu
from jax.sharding import Mesh, PartitionSpec as P


ROTARY_DIM = 64
LN_EPS = 1e-5
LANES = 128
PIECES = 2
MASKED = -1e30


def layer_norm(hidden_rows, gain_vec, bias_vec):
    rows_f32 = hidden_rows.astype(jnp.float32)
    row_mean = jnp.mean(rows_f32, axis=-1, keepdims=True)
    centered = rows_f32 - row_mean
    row_var = jnp.mean(centered * centered, axis=-1, keepdims=True)
    return (centered * lax.rsqrt(row_var + LN_EPS) * gain_vec + bias_vec).astype(jnp.bfloat16)


def norm_body(has_partial, waits, *refs):
    inputs = 5 if has_partial else 3
    refs = refs[:inputs] + refs[inputs + waits :]
    if has_partial:
        held_ref, part_ref, shift_ref, gain_ref, bias_ref, new_ref, normed_ref = refs
        rows = held_ref[...].astype(jnp.float32) + part_ref[...].astype(jnp.float32) + shift_ref[...]
        new_ref[...] = rows.astype(new_ref.dtype)
        rows = new_ref[...]
    else:
        held_ref, gain_ref, bias_ref, normed_ref = refs
        rows = held_ref[...]
    normed_ref[...] = layer_norm(rows, gain_ref[...], bias_ref[...])


def residual_norm(held, at, rows, layer, gain, bias, partial=None, shift=None, after=()):
    prompt, first = at
    d = held.shape[-1]
    block = min(rows, 128)
    held_spec = pl.BlockSpec((None, block, d), lambda i: (prompt, first // block + i, 0))
    row_spec = pl.BlockSpec((block, d), lambda i: (i, 0))
    new_spec = pl.BlockSpec((None, block, d), lambda i: (0, i, 0))
    vec_spec = lambda l: pl.BlockSpec((None, 1, d), lambda i: (l, 0, 0))
    out = [jax.ShapeDtypeStruct((rows, d), jnp.bfloat16)]
    vec = lambda a: a[:, None, :]
    operands, specs, out_specs = [held], [held_spec], [row_spec]
    if partial is not None:
        operands += [partial, vec(shift)]
        specs += [row_spec, vec_spec(layer - 1)]
        out = [jax.ShapeDtypeStruct((1, rows, d), jnp.bfloat16)] + out
        out_specs = [new_spec] + out_specs
    return pl.pallas_call(
        functools.partial(norm_body, partial is not None, len(after)),
        grid=(rows // block,),
        in_specs=specs + [vec_spec(layer)] * 2 + [pl.BlockSpec(memory_space=pl.ANY)] * len(after),
        out_specs=out_specs,
        out_shape=out,
        name="residual_norm",
        cost_estimate=pl.CostEstimate(flops=12 * rows * d, bytes_accessed=8 * rows * d, transcendentals=0),
    )(*operands, vec(gain), vec(bias), *after)


def last_body(held_ref, part_ref, shift_ref, *rest):
    rows = held_ref[...].astype(jnp.float32) + part_ref[...].astype(jnp.float32) + shift_ref[...]
    rest[-1][...] = rows.astype(rest[-1].dtype)


def last_residual(result, batch, prompt, held, first, partial, shift):
    rows, d = partial.shape
    total = held.shape[1]
    block = min(rows, 128)
    row_spec = pl.BlockSpec((block, d), lambda i: (i, 0))
    out_spec = pl.BlockSpec((None, block, d), lambda i: (prompt, first // block + i, 0))
    made = [] if result is None else [result]
    return pl.pallas_call(
        last_body,
        grid=(rows // block,),
        in_specs=[pl.BlockSpec((None, block, d), lambda i: (0, first // block + i, 0)), row_spec, pl.BlockSpec((1, d), lambda i: (0, 0))] + [pl.BlockSpec(memory_space=pl.ANY)] * len(made),
        out_specs=out_spec,
        out_shape=jax.ShapeDtypeStruct((batch, total, d), jnp.bfloat16),
        input_output_aliases={3: 0} if made else {},
        name="last_residual",
        cost_estimate=pl.CostEstimate(flops=2 * rows * d, bytes_accessed=6 * rows * d, transcendentals=0),
    )(held, partial, shift[None, :], *made)


def rotary_lanes(seq_full):
    positions = jnp.arange(seq_full).astype(jnp.float32)
    inv_freq = 10000.0 ** (-jnp.arange(0, ROTARY_DIM, 2).astype(jnp.float32) / ROTARY_DIM)
    angles = positions[:, None] * jnp.repeat(inv_freq, 2)[None, :]
    rest = ((0, 0), (0, LANES - ROTARY_DIM))
    cos_tab = jnp.pad(jnp.cos(angles), rest, constant_values=1.0)
    sin_tab = jnp.pad(jnp.sin(angles), rest)
    even = (jnp.arange(LANES) % 2 == 0)[None, :]
    return cos_tab, jnp.where(even, -sin_tab, 0.0), jnp.where(even, 0.0, sin_tab)


def qkv_body(heads, head_dim, count, *refs):
    pieces = refs[:count]
    wq_ref, wk_ref, wv_ref, cos_ref, up_ref, down_ref = refs[count : count + 6]
    q_ref, k_ref, v_ref = refs[-3:]
    rows = jnp.concatenate([piece[...] for piece in pieces], axis=0)
    assert math.frexp(head_dim**-0.5)[0] == 0.5
    for w_ref, o_ref, turned in ((wq_ref, q_ref, True), (wk_ref, k_ref, True), (wv_ref, v_ref, False)):
        projected = jnp.dot(rows, w_ref[...], preferred_element_type=jnp.float32)
        if o_ref is q_ref:
            projected = projected * head_dim**-0.5
        for head in range(heads):
            lo = head * head_dim
            if turned:
                first = projected[:, lo : lo + LANES]
                first = first * cos_ref[...] + pltpu.roll(first, LANES - 1, 1) * up_ref[...] + pltpu.roll(first, 1, 1) * down_ref[...]
                o_ref[head, :, :LANES] = first.astype(o_ref.dtype)
                o_ref[head, :, LANES:] = projected[:, lo + LANES : lo + head_dim].astype(o_ref.dtype)
            else:
                o_ref[head] = projected[:, lo : lo + head_dim].astype(o_ref.dtype)


def project_qkv(pieces, wq, wk, wv, tables, layer, heads, head_dim, after):
    devices, rows, d = pieces[0].shape
    block = rows * len(pieces)
    width = heads * head_dim
    weight_spec = pl.BlockSpec((None, d, width), lambda i: (layer, 0, 0), pipeline_mode=pl.Buffered(1))
    table_spec = pl.BlockSpec((block, LANES), lambda i: (i, 0))
    out_spec = pl.BlockSpec((heads, block, head_dim), lambda i: (0, i, 0))
    out = jax.ShapeDtypeStruct((heads, devices * block, head_dim), jnp.bfloat16)
    return pl.pallas_call(
        functools.partial(qkv_body, heads, head_dim, len(pieces)),
        grid=(devices,),
        in_specs=[pl.BlockSpec((None, rows, d), lambda i: (i, 0, 0))] * len(pieces) + [weight_spec] * 3 + [table_spec] * 3 + [pl.BlockSpec(memory_space=pl.ANY)] * len(after),
        out_specs=[out_spec] * 3,
        out_shape=[out] * 3,
        name="project_qkv",
        cost_estimate=pl.CostEstimate(flops=6 * devices * block * d * width, bytes_accessed=2 * devices * block * d + 6 * d * width + 6 * devices * block * width, transcendentals=0),
        compiler_params=pltpu.CompilerParams(dimension_semantics=("arbitrary",), vmem_limit_bytes=60 * 1024 * 1024),
    )(*pieces, wq, wk, wv, *tables, *after)


def attention_body(heads, head_dim, block, batch_idx, lengths_ref, q_ref, k_ref, v_ref, *rest):
    o_ref = rest[-1]
    length = lengths_ref[batch_idx]
    q_idx = pl.program_id(0)
    whole = jnp.minimum(q_idx, length // block)

    def scores_of(head, k_idx):
        keys = k_ref[head, pl.ds(pl.multiple_of(k_idx * block, block), block), :]
        return lax.dot_general(q_ref[head], keys, (((1,), (1,)), ((), ())), preferred_element_type=jnp.float32)

    def values_of(head, k_idx):
        return v_ref[head, pl.ds(pl.multiple_of(k_idx * block, block), block), :]

    q_pos = q_idx * block + lax.broadcasted_iota(jnp.int32, (block, block), 0)
    k_pos = whole * block + lax.broadcasted_iota(jnp.int32, (block, block), 1)
    allowed = (k_pos <= q_pos) & (k_pos < length)
    state = []
    for head, scores in enumerate([scores_of(head, whole) for head in range(heads)]):
        scores = jnp.where(allowed, scores, MASKED)
        top = jnp.max(scores, axis=1, keepdims=True)
        probs = jnp.exp(scores - top)
        total = jnp.sum(probs, axis=1, keepdims=True)
        acc = jnp.dot(probs.astype(jnp.bfloat16), values_of(head, whole), preferred_element_type=jnp.float32)
        state.append((top, total, acc))

    def step(k_idx, state):
        out = []
        all_scores = [scores_of(head, k_idx) for head in range(heads)]
        for head, (scores, (top, total, acc)) in enumerate(zip(all_scores, state)):
            new_top = jnp.maximum(top, jnp.max(scores, axis=1, keepdims=True))
            probs = jnp.exp(scores - new_top)
            shrink = jnp.exp(top - new_top)
            total = total * shrink + jnp.sum(probs, axis=1, keepdims=True)
            acc = acc * shrink + jnp.dot(probs.astype(jnp.bfloat16), values_of(head, k_idx), preferred_element_type=jnp.float32)
            out.append((new_top, total, acc))
        return tuple(out)

    state = lax.fori_loop(0, whole, step, tuple(state))
    for head, (_, total, acc) in enumerate(state):
        o_ref[:, head * head_dim : (head + 1) * head_dim] = (acc / total).astype(o_ref.dtype)


def causal_attention(lengths, query_all, keys_all, values_all, batch_idx, block, after=()):
    heads, seq, head_dim = query_all.shape
    whole_spec = pl.BlockSpec((heads, seq, head_dim), lambda i, *_: (0, 0, 0))
    return pl.pallas_call(
        functools.partial(attention_body, heads, head_dim, block, batch_idx),
        grid_spec=pltpu.PrefetchScalarGridSpec(
            num_scalar_prefetch=1,
            grid=(seq // block,),
            in_specs=[pl.BlockSpec((heads, block, head_dim), lambda i, *_: (0, i, 0)), whole_spec, whole_spec] + [pl.BlockSpec(memory_space=pl.ANY)] * len(after),
            out_specs=pl.BlockSpec((block, heads * head_dim), lambda i, *_: (i, 0)),
        ),
        out_shape=jax.ShapeDtypeStruct((seq, heads * head_dim), jnp.bfloat16),
        name="causal_attention",
        cost_estimate=pl.CostEstimate(flops=4 * heads * seq * seq * head_dim, bytes_accessed=8 * heads * seq * head_dim, transcendentals=heads * seq * seq // 2),
        compiler_params=pltpu.CompilerParams(dimension_semantics=("arbitrary",), vmem_limit_bytes=60 * 1024 * 1024),
    )(lengths, query_all, keys_all, values_all, *after)


def out_body(ctx_ref, fc_ref, wo_ref, w_ref, o_ref, send_ref, recv_ref, send_sem, recv_sem):
    n, side, h = (pl.program_id(i) for i in range(3))
    sibling = 1 - lax.axis_index("core")
    slots = recv_ref.shape[0] - 1

    def exchange(half):
        slot = n * 2 + half
        return pltpu.make_async_remote_copy(
            src_ref=send_ref.at[half], dst_ref=recv_ref.at[slot], send_sem=send_sem.at[half], recv_sem=recv_sem.at[slot], device_id={"core": sibling}, device_id_type=pl.DeviceIdType.MESH
        )

    @pl.when((n == 0) & (side == 0) & (h == 0))
    def _():
        recv_ref[slots] = jnp.zeros(recv_ref.shape[1:], recv_ref.dtype)
        barrier = pltpu.get_barrier_semaphore()
        pl.semaphore_signal(barrier, inc=1, device_id={"core": sibling}, device_id_type=pl.DeviceIdType.MESH)
        pl.semaphore_wait(barrier, 1)

    @pl.when((side == 0) & (h == 1))
    def _():
        exchange(0).start()

    @pl.when((side == 1) & (h == 0))
    def _():
        exchange(1).start()
        exchange(0).wait()

    @pl.when((side == 1) & (h == 1))
    def _():
        exchange(1).wait()

    groups, rows, width = ctx_ref.shape
    cols = o_ref.shape[-1] // 4
    fc = fc_ref[...].reshape(groups * rows, fc_ref.shape[-1])
    ctx = ctx_ref[...].reshape(groups * rows, width)
    slot = jnp.where(side == 1, n * 2 + h, slots)
    for part in range(4):
        at = slice(part * cols, (part + 1) * cols)
        total = jnp.dot(fc, w_ref[:, at], preferred_element_type=jnp.float32)
        total += jnp.dot(ctx, wo_ref[:, at], preferred_element_type=jnp.float32)
        send_ref[h, :, at] = total.astype(send_ref.dtype)
        both = total + recv_ref[slot, :, at].astype(jnp.float32)
        o_ref[:, :, at] = both.astype(o_ref.dtype).reshape(groups, rows, cols)


def project_out(context, fc_hidden, wo, w_out, layer, piece, collective_id):
    chips, cores, _, rows, width = context.shape
    ff = fc_hidden.shape[-1]
    d = wo.shape[-1]
    group = chips // 2
    cols = 1024
    block = group * rows
    slots = d // cols * 2

    def core_of(side):
        return lax.rem(lax.axis_index("core") + 1 + side, 2)

    work = chips * cores * rows
    return pl.pallas_call(
        out_body,
        grid=(d // cols, cores, 2),
        in_specs=[
            pl.BlockSpec((group, None, None, rows, width), lambda n, s, h: (h, core_of(s), piece, 0, 0)),
            pl.BlockSpec((group, None, None, rows, ff), lambda n, s, h: (h, core_of(s), 0, 0, 0)),
            pl.BlockSpec((None, width, cols), lambda n, s, h: (layer, 0, n)),
            pl.BlockSpec((None, ff, cols), lambda n, s, h: (layer, 0, n)),
        ],
        out_specs=pl.BlockSpec((group, rows, cols), lambda n, s, h: (h * s, 0, n)),
        out_shape=jax.ShapeDtypeStruct((chips, rows, d), jnp.bfloat16),
        scratch_shapes=[
            pltpu.VMEM((2, block, cols), jnp.bfloat16),
            pltpu.VMEM((slots + 1, block, cols), jnp.bfloat16),
            pltpu.SemaphoreType.DMA((2,)),
            pltpu.SemaphoreType.DMA((slots,)),
        ],
        name="project_out",
        cost_estimate=pl.CostEstimate(flops=2 * work * (ff + width) * d, bytes_accessed=2 * (work * (ff + width + d) + (ff + width) * d), transcendentals=0),
        compiler_params=pltpu.CompilerParams(dimension_semantics=("arbitrary",) * 3, vmem_limit_bytes=63 * 1024 * 1024, collective_id=collective_id, has_side_effects=True),
    )(context, fc_hidden, wo, w_out)


def solution(mesh):
    tp_size = mesh.shape["tp"]
    mesh = Mesh(mesh.devices.reshape(mesh.shape["dp"], tp_size // 2, 2), ("dp", "chip", "core"))
    tp = ("chip", "core")

    def device_step(hidden, lengths, ln_gain, ln_bias, w_query, w_key, w_value, w_attn_out, w_fc_in, b_fc_in, w_fc_out, b_fc_out):
        batch, rows_own, d = hidden.shape
        layers, _, heads, head_dim = w_query.shape
        seq_full = rows_own * tp_size
        tables = rotary_lanes(seq_full)
        wq, wk, wv = (w.reshape(layers, d, heads * head_dim) for w in (w_query, w_key, w_value))
        wo = w_attn_out.reshape(layers, heads * head_dim, d)
        chips = tp_size // 2

        def pieces_of(layer, b):
            return PIECES if (layer, b) in ((0, 0), (layers - 1, batch - 1)) else 1

        def gather(normed, layer, b):
            count = pieces_of(layer, b)
            rows = rows_own // count
            if len(normed) < count:
                normed = [normed[0][piece * rows : (piece + 1) * rows] for piece in range(count)]
            gathered = []
            for piece in range(count):
                gathered.append(lax.all_gather(normed[piece], tp, axis=0))
            return gathered

        def fc_in(rows, layer):
            return jax.nn.gelu(jnp.einsum("ntd,df->ntf", rows, w_fc_in[layer], preferred_element_type=jnp.float32) + b_fc_in[layer], approximate=True).astype(jnp.bfloat16)

        stages = [(layer, b) for layer in range(layers) for b in range(batch)]
        held = [(hidden, b) for b in range(batch)]
        normed = []
        for b in range(batch):
            count = pieces_of(0, b)
            rows = rows_own // count
            normed.append([residual_norm(hidden, (b, piece * rows), rows, 0, ln_gain, ln_bias, after=normed[-1] if normed else ())[0] for piece in range(count)])
        gathered = [gather(normed[b], 0, b) for b in range(batch)]
        cache_k = []
        cache_v = []
        result = None
        waiting = None
        for layer, b in stages:
            pieces = pieces_of(layer, b)
            rows = rows_own // pieces
            first_fc = fc_in(gathered[b][0], layer)

            def qkv(after):
                return project_qkv(gathered[b], wq, wk, wv, tables, layer, heads, head_dim, after)

            early = waiting is None or pieces_of(*waiting[:2]) > 1
            if not early:
                query_all, keys_all, values_all = qkv([first_fc])
            moved = []
            if waiting is not None:
                up, prompt, sums = waiting
                if up < layers - 1:
                    after = [first_fc] if early else [first_fc, query_all]
                    array, place = held[prompt]
                    new, normed_rows = residual_norm(array, (place, 0), rows_own, up + 1, ln_gain, ln_bias, jnp.concatenate(sums, axis=0), b_fc_out, after)
                    held[prompt] = (new, 0)
                    gathered[prompt] = gather([normed_rows], up + 1, prompt)
                    moved = [normed_rows]
                else:
                    result = last_residual(result, batch, prompt, held[prompt][0], 0, jnp.concatenate(sums, axis=0), b_fc_out[up])
            if early:
                query_all, keys_all, values_all = qkv([first_fc] + moved)
            cache_k.append(keys_all)
            cache_v.append(values_all)
            context = causal_attention(lengths, query_all, keys_all, values_all, b, rows_own, moved)
            context = context.reshape(chips, 2, pieces, rows, heads * head_dim)
            sums = []
            part = None
            for piece in range(pieces):
                if piece == 0:
                    fc = first_fc
                else:
                    source, _ = lax.optimization_barrier((gathered[b][piece], part))
                    fc = fc_in(source, layer)
                fc = fc.reshape(chips, 2, 1, rows, -1)
                part = project_out(context, fc, wo, w_fc_out, layer, piece, (layer * batch + b) * PIECES + piece)
                sums.append(lax.psum_scatter(part, "chip", scatter_dimension=0))
            waiting = (layer, b, sums)
        layer, b, sums = waiting
        for piece, part in enumerate(sums):
            result = last_residual(result, batch, b, held[b][0], piece * (rows_own // len(sums)), part, b_fc_out[layer])
        cache_shape = (layers, batch, heads, seq_full, head_dim)
        return result, jnp.stack(cache_k).reshape(cache_shape), jnp.stack(cache_v).reshape(cache_shape)

    head_cols = P(None, None, tp, None)
    cache_spec = P(None, "dp", tp, None, None)
    hidden_spec = P("dp", tp, None)
    return jax.shard_map(device_step, mesh=mesh, in_specs=(hidden_spec, P("dp"), P(), P(), head_cols, head_cols, head_cols, P(None, tp, None, None), P(None, None, tp), P(None, tp), P(None, tp, None), P()), out_specs=(hidden_spec, cache_spec, cache_spec), check_vma=False)
```
